16 devices in a mesh: dp: 2 (over y, z), cp: 8 (over x, core).
Axes of the slice: x: 4, y: 2, z: 1, core: 2. Of those that a mesh axis runs over, the one named last changes fastest.
The devices are a block of a 4x4x8 slice.
Arguments:
- hidden: bfloat16 [32, 2048, 5120], P('dp', 'cp'), parts along dimension 0
- positions: int32 [32, 2048], P('dp', 'cp'), parts along dimension 0
- w_q: bfloat16 [5120, 32, 128], replicated
- w_k: bfloat16 [5120, 8, 128], replicated
- w_v: bfloat16 [5120, 8, 128], replicated
- w_o: bfloat16 [32, 128, 5120], replicated
Outputs:
- output: bfloat16 [32, 2048, 5120], P('dp', 'cp'), parts along dimension 0
There are 2 independent parts. The reference program is written for one: setup_inputs(seed, part) draws one part's arguments, and reference() takes and returns one part's arrays. A program takes and returns all parts, laid end to end along the dimension named above; an argument that names none is the same for every part.
All inputs are finite; a program needn't handle non-finite values.
Results may differ from the reference program's by a relative error of at most 0.00862.
Values are sent between devices in bfloat16 or wider.
A program may use at most 768 MiB of HBM per device.

```python
import jax
import jax.numpy as jnp
from jax import lax

BATCH = 16
SEQ = 2048
D = 5120
HEADS = 32
KV_HEADS = 8
HEAD = 128

ROPE_BASE = 500000.0
Q_PER_KV = HEADS // KV_HEADS


def setup_inputs(seed: int = 0, part: int = 0) -> dict:
    part_key = jax.random.fold_in(jax.random.key(seed), part)
    k_noise, k_coef, k_phase, k_step, k_first = jax.random.split(part_key, 5)
    k_wq, k_wk, k_wv, k_wo = jax.random.split(jax.random.key(seed + 1), 4)
    time_grid = jnp.arange(SEQ, dtype=jnp.float32) / SEQ
    mode_ids = jnp.arange(1, 5, dtype=jnp.float32)
    phases = jax.random.uniform(k_phase, (BATCH, 4), jnp.float32, 0.0, 6.2831853)
    wave_vals = jnp.cos(6.2831853 * time_grid[None, :, None] * mode_ids[None, None, :] + phases[:, None, :])
    mode_coef = 0.6 * jax.random.normal(k_coef, (BATCH, 4, D), jnp.float32)
    slow_part = jnp.einsum('bsm,bmd->bsd', wave_vals, mode_coef)
    noise_part = 0.6 * jax.random.normal(k_noise, (BATCH, SEQ, D), jnp.float32)
    hidden = (slow_part + noise_part).astype(jnp.bfloat16)
    step_sizes = jax.random.randint(k_step, (BATCH, SEQ), 1, 5)
    first_pos = jax.random.randint(k_first, (BATCH, 1), 0, 4)
    positions = (first_pos + jnp.cumsum(step_sizes, axis=1) - step_sizes[:, :1]).astype(jnp.int32)
    w_q = (jax.random.normal(k_wq, (D, HEADS, HEAD), jnp.float32) * D ** -0.5).astype(jnp.bfloat16)
    w_k = (jax.random.normal(k_wk, (D, KV_HEADS, HEAD), jnp.float32) * D ** -0.5).astype(jnp.bfloat16)
    w_v = (jax.random.normal(k_wv, (D, KV_HEADS, HEAD), jnp.float32) * (2.0 * D ** -0.5)).astype(jnp.bfloat16)
    w_o = (jax.random.normal(k_wo, (HEADS, HEAD, D), jnp.float32) * (HEADS * HEAD) ** -0.5).astype(jnp.bfloat16)
    return {'hidden': hidden, 'positions': positions, 'w_q': w_q, 'w_k': w_k, 'w_v': w_v, 'w_o': w_o}


def rope_tables(positions):
    inv_freq = ROPE_BASE ** (-jnp.arange(0, HEAD, 2, dtype=jnp.float32) / HEAD)
    angles = positions.astype(jnp.float32)[..., None] * inv_freq
    angles = jnp.concatenate([angles, angles], axis=-1)
    return jnp.cos(angles)[:, :, None, :], jnp.sin(angles)[:, :, None, :]


def rope_apply(in_vals, cos_tab, sin_tab):
    half_dim = in_vals.shape[-1] // 2
    val_f32 = in_vals.astype(jnp.float32)
    rotated = jnp.concatenate([-val_f32[..., half_dim:], val_f32[..., :half_dim]], axis=-1)
    return (val_f32 * cos_tab + rotated * sin_tab).astype(jnp.bfloat16)


def reference(hidden, positions, w_q, w_k, w_v, w_o):
    x_float = hidden.astype(jnp.float32)
    queries = jnp.einsum('bsd,dhe->bshe', x_float, w_q.astype(jnp.float32)).astype(jnp.bfloat16)
    k_proj = jnp.einsum('bsd,dhe->bshe', x_float, w_k.astype(jnp.float32)).astype(jnp.bfloat16)
    values = jnp.einsum('bsd,dhe->bshe', x_float, w_v.astype(jnp.float32)).astype(jnp.bfloat16)
    cos_tab, sin_tab = rope_tables(positions)
    queries = rope_apply(queries, cos_tab, sin_tab)
    k_rot = rope_apply(k_proj, cos_tab, sin_tab)
    q_block = 16
    n_blocks = SEQ // q_block
    q_blocks = queries.reshape(BATCH, n_blocks, q_block, KV_HEADS, Q_PER_KV, HEAD).transpose(1, 0, 2, 3, 4, 5)
    pos_blocks = positions.reshape(BATCH, n_blocks, q_block).transpose(1, 0, 2)
    k_float = k_rot.astype(jnp.float32)
    v_float = values.astype(jnp.float32)
    sm_scale = HEAD ** -0.5

    def one_block(block_args):
        q_blk, pos_blk = block_args
        scores = jnp.einsum('bqkge,bske->bkgqs', q_blk.astype(jnp.float32), k_float) * sm_scale
        allowed = positions[:, None, None, None, :] <= pos_blk[:, None, None, :, None]
        scores = jnp.where(allowed, scores, -jnp.inf)
        row_max = jnp.max(scores, axis=-1, keepdims=True)
        p_weights = jnp.exp(scores - row_max)
        row_sum = jnp.sum(p_weights, axis=-1)
        out_acc = jnp.einsum('bkgqs,bske->bqkge', p_weights.astype(jnp.bfloat16).astype(jnp.float32), v_float)
        return (out_acc / row_sum.transpose(0, 3, 1, 2)[..., None]).astype(jnp.bfloat16)

    attn_blocks = lax.map(one_block, (q_blocks, pos_blocks))
    attn_out = attn_blocks.transpose(1, 0, 2, 3, 4, 5).reshape(BATCH, SEQ, HEADS, HEAD)
    proj_out = jnp.einsum('bshe,hed->bsd', attn_out.astype(jnp.float32), w_o.astype(jnp.float32))
    return (x_float + proj_out).astype(jnp.bfloat16)
```

```python
import functools

import jax
import jax.numpy as jnp
from jax import lax
from jax.experimental import pallas as pl
from jax.experimental.pallas import tpu as pltpu
from jax.experimental.layout import Layout, with_layout_constraint
from jax.sharding import PartitionSpec as P

ROPE_BASE = 500000.0
LOG2E = 1.4426950408889634
N_CHUNKS = 2


def VARIANTS(n_dev):
    return sorted({max(n_dev // 2 - 1, 1), max(n_dev - 1, 1), n_dev})


def rope_tables(positions, head_dim):
    half = head_dim // 2
    inv_freq = ROPE_BASE ** (-jnp.arange(0, head_dim, 2, dtype=jnp.float32) / head_dim)
    angles = positions.astype(jnp.float32)[..., None] * inv_freq
    angles = jnp.concatenate([angles, angles], axis=-1)
    sign = jnp.where(jnp.arange(head_dim) < half, -1.0, 1.0).astype(jnp.float32)
    return jnp.cos(angles), jnp.sin(angles) * sign


def rope_block(val, cos_tab, sin_tab):
    v = val.astype(jnp.float32)
    return (v * cos_tab + pltpu.roll(v, v.shape[-1] // 2, v.ndim - 1) * sin_tab).astype(jnp.bfloat16)


def k_rope_kernel(k_ref, cos_ref, sin_ref, o_ref):
    cos_tab, sin_tab = cos_ref[0], sin_ref[0]
    for g in range(k_ref.shape[1]):
        o_ref[0, g] = rope_block(k_ref[0, g], cos_tab, sin_tab)


def k_rope(k_proj, cos_tab, sin_tab):
    nb, n_kv, tok, hd = k_proj.shape
    tab = pl.BlockSpec((1, tok, hd), lambda b: (b, 0, 0))
    blk = pl.BlockSpec((1, n_kv, tok, hd), lambda b: (b, 0, 0, 0))
    return pl.pallas_call(
        k_rope_kernel,
        grid=(nb,),
        in_specs=[blk, tab, tab],
        out_specs=blk,
        out_shape=jax.ShapeDtypeStruct(k_proj.shape, jnp.bfloat16),
        cost_estimate=pl.CostEstimate(flops=nb * n_kv * tok * hd * 400, bytes_accessed=nb * n_kv * tok * hd * 4, transcendentals=0),
    )(k_proj, cos_tab, sin_tab)


def attn_kernel(n_ref, q_ref, k_ref, v_ref, cos_ref, sin_ref, o_ref, qa, qb, sa, sb, pa, pb, la, lb, *, n_dev, q_per_kv):
    n_heads, tok, hd = q_ref.shape[1], q_ref.shape[2], q_ref.shape[3]
    n_pairs = n_heads // 2
    c = (hd ** -0.5) * LOG2E
    row_chunk = 64

    def rope_stage(i, q_scr):
        cos_tab, sin_tab = cos_ref[0], sin_ref[0]
        for t in range(2):
            q_scr[pl.ds(t * tok, tok), :] = rope_block(q_ref[0, 2 * i + t], cos_tab, sin_tab)

    def qk_stage(i, q_scr, s_scr, n):
        g = (2 * i) // q_per_kv
        q = q_scr[...]
        for j in range(n):
            s_scr[:, j * tok:(j + 1) * tok] = lax.dot_general(
                q, k_ref[j, 0, g], (((1,), (1,)), ((), ())), preferred_element_type=jnp.float32)

    def softmax_stage(s_scr, p_scr, l_scr, n, first_masked, me):
        for r in range(0, 2 * tok, row_chunk):
            rows = pl.ds(r, row_chunk)
            ri = lax.broadcasted_iota(jnp.int32, (row_chunk, tok), 0) + (r % tok)
            diff = lax.broadcasted_iota(jnp.int32, (row_chunk, tok), 1) - ri

            def scores(j):
                val = s_scr[rows, j * tok:(j + 1) * tok]
                if j < first_masked:
                    return val
                limit = 0 if first_masked == n - 1 else (me - j) * tok
                return jnp.where(diff <= limit, val, -jnp.inf)

            mx = scores(0)
            for j in range(1, n):
                mx = jnp.maximum(mx, scores(j))
            mx = jnp.max(mx, axis=1, keepdims=True)
            tot = None
            for j in range(n):
                pj = jnp.exp2((scores(j) - mx) * c)
                p_scr[rows, j * tok:(j + 1) * tok] = pj.astype(jnp.bfloat16)
                part = pj[:, :hd] + pj[:, hd:]
                tot = part if tot is None else tot + part
            l_scr[rows, :] = jnp.broadcast_to(jnp.sum(tot, axis=1, keepdims=True), (row_chunk, hd))

    def pv_stage(i, p_scr, l_scr, n):
        g = (2 * i) // q_per_kv
        acc = None
        for j in range(n):
            part = jnp.dot(p_scr[:, j * tok:(j + 1) * tok], v_ref[j, 0, g], preferred_element_type=jnp.float32)
            acc = part if acc is None else acc + part
        out = (acc / l_scr[...]).astype(jnp.bfloat16)
        for t in range(2):
            o_ref[0, :, pl.ds(pl.multiple_of((2 * i + t) * hd, hd), hd)] = out[t * tok:(t + 1) * tok]

    def run(n, lo):
        last_pair = n_pairs - 1
        rope_stage(0, qa)
        qk_stage(0, qa, sa, n)
        rope_stage(1, qb)

        def body(it, _):
            i = 2 * it
            prev = jnp.maximum(i - 1, 0)
            qk_stage(i + 1, qb, sb, n)
            rope_stage(jnp.minimum(i + 2, last_pair), qa)
            softmax_stage(sa, pa, la, n, lo - 1, me)
            pv_stage(prev, pb, lb, n)
            qk_stage(jnp.minimum(i + 2, last_pair), qa, sa, n)
            rope_stage(jnp.minimum(i + 3, last_pair), qb)
            softmax_stage(sb, pb, lb, n, lo - 1, me)
            pv_stage(i, pa, la, n)
            return 0

        lax.fori_loop(0, n_pairs // 2, body, 0)
        pv_stage(last_pair, pb, lb, n)

    me = n_ref[0]
    lo = 1
    for n in VARIANTS(n_dev):
        pl.when((me + 1 >= lo) & (me < n))(functools.partial(run, n, lo))
        lo = n + 1


def attention(n_act, q, k_all, v_all, cos_tab, sin_tab):
    nb, n_heads, tok, hd = q.shape
    n_dev, _, n_kv = k_all.shape[:3]
    tab = pl.BlockSpec((1, tok, hd), lambda b, *_: (b, 0, 0))
    kv = pl.BlockSpec((n_dev, 1, n_kv, tok, hd), lambda b, *_: (0, b, 0, 0, 0))
    keys = n_dev * tok
    macs = nb * n_heads * tok * keys * hd
    return pl.pallas_call(
        functools.partial(attn_kernel, n_dev=n_dev, q_per_kv=n_heads // n_kv),
        grid_spec=pltpu.PrefetchScalarGridSpec(
            num_scalar_prefetch=1,
            grid=(nb,),
            in_specs=[pl.BlockSpec((1, n_heads, tok, hd), lambda b, *_: (b, 0, 0, 0)), kv, kv, tab, tab],
            out_specs=pl.BlockSpec((1, tok, n_heads * hd), lambda b, *_: (b, 0, 0)),
            scratch_shapes=[
                pltpu.VMEM((2 * tok, hd), jnp.bfloat16), pltpu.VMEM((2 * tok, hd), jnp.bfloat16),
                pltpu.VMEM((2 * tok, keys), jnp.float32), pltpu.VMEM((2 * tok, keys), jnp.float32),
                pltpu.VMEM((2 * tok, keys), jnp.bfloat16), pltpu.VMEM((2 * tok, keys), jnp.bfloat16),
                pltpu.VMEM((2 * tok, hd), jnp.float32), pltpu.VMEM((2 * tok, hd), jnp.float32),
            ],
        ),
        out_shape=jax.ShapeDtypeStruct((nb, tok, n_heads * hd), jnp.bfloat16),
        compiler_params=pltpu.CompilerParams(vmem_limit_bytes=60 * 1024 * 1024),
        cost_estimate=pl.CostEstimate(flops=8 * macs, bytes_accessed=2 * (2 * q.size + 2 * k_all.size), transcendentals=0),
    )(n_act, q, k_all, v_all, cos_tab, sin_tab)


def solution(mesh):
    def per_device(hidden, positions, w_q, w_k, w_v, w_o):
        n_batch, tok = hidden.shape[0], hidden.shape[1]
        n_act = lax.axis_index('cp').astype(jnp.int32).reshape(1)
        cos_tab, sin_tab = rope_tables(positions, w_q.shape[2])
        cb = n_batch // N_CHUNKS
        spans = [slice(i * cb, (i + 1) * cb) for i in range(N_CHUNKS)]

        def proj(x, w):
            return jnp.einsum('bsd,dhe->bshe', x, w, preferred_element_type=jnp.float32).astype(jnp.bfloat16).transpose(0, 2, 1, 3)

        k_all, v_all = [], []
        for sp in spans:
            kr = k_rope(proj(hidden[sp], w_k), cos_tab[sp], sin_tab[sp])
            k_all.append(lax.all_gather(kr, 'cp'))
            v_all.append(lax.all_gather(with_layout_constraint(proj(hidden[sp], w_v), Layout((0, 1, 2, 3))), 'cp'))
        w_o2 = w_o.reshape(-1, w_o.shape[2])
        outs = []
        for i, sp in enumerate(spans):
            q = proj(hidden[sp], w_q)
            attn = attention(n_act, q, k_all[i], v_all[i], cos_tab[sp], sin_tab[sp])
            y = jnp.einsum('bsf,fd->bsd', attn, w_o2, preferred_element_type=jnp.float32)
            outs.append((hidden[sp].astype(jnp.float32) + y).astype(jnp.bfloat16))
        return jnp.concatenate(outs, axis=0)

    rep = P(None, None, None)
    return jax.shard_map(per_device, mesh=mesh, in_specs=(P('dp', 'cp', None), P('dp', 'cp'), rep, rep, rep, rep), out_specs=P('dp', 'cp', None), check_vma=False)
```

```python
import functools

import jax
import jax.numpy as jnp
from jax import lax
from jax.experimental import pallas as pl
from jax.experimental.pallas import tpu as pltpu
from jax.experimental.layout import Layout, with_layout_constraint
from jax.sharding import PartitionSpec as P

ROPE_BASE = 500000.0
LOG2E = 1.4426950408889634
CHUNK_PARTS = (3, 3, 2)


def VARIANTS(n_dev):
    return sorted({max(n_dev // 2 - 1, 1), max(n_dev - 1, 1), n_dev})


def rope_tables(positions, head_dim):
    half = head_dim // 2
    inv_freq = ROPE_BASE ** (-jnp.arange(0, head_dim, 2, dtype=jnp.float32) / head_dim)
    angles = positions.astype(jnp.float32)[..., None] * inv_freq
    angles = jnp.concatenate([angles, angles], axis=-1)
    sign = jnp.where(jnp.arange(head_dim) < half, -1.0, 1.0).astype(jnp.float32)
    return jnp.cos(angles), jnp.sin(angles) * sign


def rope_block(val, cos_tab, sin_tab):
    v = val.astype(jnp.float32)
    return (v * cos_tab + pltpu.roll(v, v.shape[-1] // 2, v.ndim - 1) * sin_tab).astype(jnp.bfloat16)


def k_rope_kernel(k_ref, cos_ref, sin_ref, o_ref):
    for b in range(k_ref.shape[0]):
        cos_tab, sin_tab = cos_ref[b], sin_ref[b]
        for g in range(k_ref.shape[1]):
            o_ref[b, g] = rope_block(k_ref[b, g], cos_tab, sin_tab)


def k_rope(k_proj, cos_tab, sin_tab):
    nb, n_kv, tok, hd = k_proj.shape
    bb = 2 if nb % 2 == 0 else 1
    tab = pl.BlockSpec((bb, tok, hd), lambda b: (b, 0, 0))
    blk = pl.BlockSpec((bb, n_kv, tok, hd), lambda b: (b, 0, 0, 0))
    return pl.pallas_call(
        k_rope_kernel,
        grid=(nb // bb,),
        in_specs=[blk, tab, tab],
        out_specs=blk,
        out_shape=jax.ShapeDtypeStruct(k_proj.shape, jnp.bfloat16),
        cost_estimate=pl.CostEstimate(flops=nb * n_kv * tok * hd * 400, bytes_accessed=nb * n_kv * tok * hd * 4, transcendentals=0),
    )(k_proj, cos_tab, sin_tab)


def attn_kernel(n_ref, q_ref, k_ref, v_ref, cos_ref, sin_ref, o_ref, qa, qb, sa, sb, pa, pb, la, lb, vt, *, n_dev, q_per_kv):
    n_heads, tok, hd = q_ref.shape[1], q_ref.shape[2], q_ref.shape[3]
    n_pairs = n_heads // 2
    c = (hd ** -0.5) * LOG2E
    row_chunk = 32
    assert q_per_kv == 4

    def rope_stage(i, q_scr):
        cos_tab, sin_tab = cos_ref[0], sin_ref[0]
        for t in range(2):
            q_scr[pl.ds(t * tok, tok), :] = rope_block(q_ref[0, 2 * i + t], cos_tab, sin_tab)

    def vt_stage(i, n):
        g = (2 * i) // q_per_kv
        for j in range(n):
            vt[:, j * tok:(j + 1) * tok] = v_ref[j, 0, g].T

    def qk_stage(i, q_scr, s_scr, n):
        g = (2 * i) // q_per_kv
        s_scr[:n * tok, :] = lax.dot_general(
            k_ref[:n, 0, g].reshape(n * tok, hd), q_scr[...], (((1,), (1,)), ((), ())), preferred_element_type=jnp.float32)

    def softmax_stage(s_scr, p_scr, l_scr, n, first_masked, me):
        for t in range(2):
            cols = slice(t * tok, (t + 1) * tok)
            diff = lax.broadcasted_iota(jnp.int32, (row_chunk, tok), 0) - lax.broadcasted_iota(jnp.int32, (row_chunk, tok), 1)

            def scores(r):
                val = s_scr[r:r + row_chunk, cols]
                j = r // tok
                if j < first_masked:
                    return val
                limit = -(r % tok) if first_masked == n - 1 else me * tok - r
                return jnp.where(diff <= limit, val, -jnp.inf)

            mx = scores(0)
            for r in range(row_chunk, n * tok, row_chunk):
                mx = jnp.maximum(mx, scores(r))
            mx = jnp.max(mx, axis=0, keepdims=True)
            tot = None
            for r in range(0, n * tok, row_chunk):
                pj = jnp.exp2((scores(r) - mx) * c)
                p_scr[r:r + row_chunk, cols] = pj.astype(jnp.bfloat16)
                tot = pj if tot is None else tot + pj
            l_scr[:, cols] = jnp.broadcast_to(jnp.sum(tot, axis=0, keepdims=True), (8, tok))

    def pv_stage(i, p_scr, l_scr, n):
        acc = jnp.dot(vt[:, :n * tok], p_scr[:n * tok, :], preferred_element_type=jnp.float32)
        out = acc * (1.0 / l_scr[0:1, :])
        for t in range(2):
            o_ref[0, :, pl.ds(pl.multiple_of((2 * i + t) * hd, hd), hd)] = out[:, t * tok:(t + 1) * tok].T.astype(jnp.bfloat16)

    def run(n, lo):
        last_pair = n_pairs - 1
        rope_stage(0, qa)
        qk_stage(0, qa, sa, n)
        rope_stage(1, qb)

        def body(it, _):
            i = 2 * it
            prev = jnp.maximum(i - 1, 0)
            qk_stage(i + 1, qb, sb, n)
            rope_stage(jnp.minimum(i + 2, last_pair), qa)
            softmax_stage(sa, pa, la, n, lo - 1, me)
            pv_stage(prev, pb, lb, n)
            vt_stage(i, n)
            qk_stage(jnp.minimum(i + 2, last_pair), qa, sa, n)
            rope_stage(jnp.minimum(i + 3, last_pair), qb)
            softmax_stage(sb, pb, lb, n, lo - 1, me)
            pv_stage(i, pa, la, n)
            return 0

        lax.fori_loop(0, n_pairs // 2, body, 0)
        pv_stage(last_pair, pb, lb, n)

    me = n_ref[0]
    lo = 1
    for n in VARIANTS(n_dev):
        pl.when((me + 1 >= lo) & (me < n))(functools.partial(run, n, lo))
        lo = n + 1


def attention(n_act, q, k_all, v_all, cos_tab, sin_tab):
    nb, n_heads, tok, hd = q.shape
    n_dev, _, n_kv = k_all.shape[:3]
    tab = pl.BlockSpec((1, tok, hd), lambda b, *_: (b, 0, 0))
    kv = pl.BlockSpec((n_dev, 1, n_kv, tok, hd), lambda b, *_: (0, b, 0, 0, 0))
    keys = n_dev * tok
    macs = nb * n_heads * tok * keys * hd
    return pl.pallas_call(
        functools.partial(attn_kernel, n_dev=n_dev, q_per_kv=n_heads // n_kv),
        grid_spec=pltpu.PrefetchScalarGridSpec(
            num_scalar_prefetch=1,
            grid=(nb,),
            in_specs=[pl.BlockSpec((1, n_heads, tok, hd), lambda b, *_: (b, 0, 0, 0)), kv, kv, tab, tab],
            out_specs=pl.BlockSpec((1, tok, n_heads * hd), lambda b, *_: (b, 0, 0)),
            scratch_shapes=[
                pltpu.VMEM((2 * tok, hd), jnp.bfloat16), pltpu.VMEM((2 * tok, hd), jnp.bfloat16),
                pltpu.VMEM((keys, 2 * tok), jnp.float32), pltpu.VMEM((keys, 2 * tok), jnp.float32),
                pltpu.VMEM((keys, 2 * tok), jnp.bfloat16), pltpu.VMEM((keys, 2 * tok), jnp.bfloat16),
                pltpu.VMEM((8, 2 * tok), jnp.float32), pltpu.VMEM((8, 2 * tok), jnp.float32),
                pltpu.VMEM((hd, keys), jnp.bfloat16),
            ],
        ),
        out_shape=jax.ShapeDtypeStruct((nb, tok, n_heads * hd), jnp.bfloat16),
        compiler_params=pltpu.CompilerParams(vmem_limit_bytes=60 * 1024 * 1024),
        cost_estimate=pl.CostEstimate(flops=8 * macs, bytes_accessed=2 * (2 * q.size + 2 * k_all.size), transcendentals=0),
    )(n_act, q, k_all, v_all, cos_tab, sin_tab)


def blank(shape, dtype):
    return pl.pallas_call(lambda o_ref: None, out_specs=pl.BlockSpec(memory_space=pl.ANY), out_shape=jax.ShapeDtypeStruct(shape, dtype))()


def solution(mesh):
    def per_device(hidden, positions, w_q, w_k, w_v, w_o):
        n_batch, tok = hidden.shape[0], hidden.shape[1]
        n_act = lax.axis_index('cp').astype(jnp.int32).reshape(1)
        cos_tab, sin_tab = rope_tables(positions, w_q.shape[2])
        unit = n_batch // sum(CHUNK_PARTS)
        ends = [unit * sum(CHUNK_PARTS[:i + 1]) for i in range(len(CHUNK_PARTS))]
        spans = [slice(e - unit * p, e) for e, p in zip(ends, CHUNK_PARTS)]

        def proj(x, w):
            return jnp.einsum('bsd,dhe->bshe', x, w, preferred_element_type=jnp.float32).astype(jnp.bfloat16).transpose(0, 2, 1, 3)

        k_all, v_all = [], []
        for sp in spans:
            kr = k_rope(proj(hidden[sp], w_k), cos_tab[sp], sin_tab[sp])
            k_all.append(lax.all_gather(kr, 'cp'))
            v_all.append(lax.all_gather(with_layout_constraint(proj(hidden[sp], w_v), Layout((0, 1, 2, 3))), 'cp'))
        w_o2 = w_o.reshape(-1, w_o.shape[2])
        out = blank(hidden.shape, hidden.dtype)
        for i, sp in enumerate(spans):
            q = proj(hidden[sp], w_q)
            attn = attention(n_act, q, k_all[i], v_all[i], cos_tab[sp], sin_tab[sp])
            y = jnp.einsum('bsf,fd->bsd', attn, w_o2, preferred_element_type=jnp.float32)
            y = (hidden[sp].astype(jnp.float32) + y).astype(jnp.bfloat16)
            out = lax.dynamic_update_slice(out, y, (sp.start, 0, 0))
        return out

    rep = P(None, None, None)
    return jax.shard_map(per_device, mesh=mesh, in_specs=(P('dp', 'cp', None), P('dp', 'cp'), rep, rep, rep, rep), out_specs=P('dp', 'cp', None), check_vma=False)
```

```python
import functools

import jax
import jax.numpy as jnp
from jax import lax
from jax.experimental import pallas as pl
from jax.experimental.pallas import tpu as pltpu
from jax.experimental.layout import Layout, with_layout_constraint
from jax.sharding import PartitionSpec as P

ROPE_BASE = 500000.0
LOG2E = 1.4426950408889634
CHUNK_PARTS = (3, 3, 2)


def VARIANTS(n_dev):
    return sorted({max(n_dev // 2 - 1, 1), max(n_dev - 1, 1), n_dev})


def rope_tables(positions, head_dim):
    half = head_dim // 2
    inv_freq = ROPE_BASE ** (-jnp.arange(0, head_dim, 2, dtype=jnp.float32) / head_dim)
    angles = positions.astype(jnp.float32)[..., None] * inv_freq
    angles = jnp.concatenate([angles, angles], axis=-1)
    sign = jnp.where(jnp.arange(head_dim) < half, -1.0, 1.0).astype(jnp.float32)
    return jnp.cos(angles), jnp.sin(angles) * sign


def rope_block(val, cos_tab, sin_tab):
    v = val.astype(jnp.float32)
    return (v * cos_tab + pltpu.roll(v, v.shape[-1] // 2, v.ndim - 1) * sin_tab).astype(jnp.bfloat16)


def k_rope_kernel(k_ref, cos_ref, sin_ref, o_ref):
    for b in range(k_ref.shape[0]):
        cos_tab, sin_tab = cos_ref[b], sin_ref[b]
        for g in range(k_ref.shape[1]):
            o_ref[b, g] = rope_block(k_ref[b, g], cos_tab, sin_tab)


def k_rope(k_proj, cos_tab, sin_tab):
    nb, n_kv, tok, hd = k_proj.shape
    bb = 2 if nb % 2 == 0 else 1
    tab = pl.BlockSpec((bb, tok, hd), lambda b: (b, 0, 0))
    blk = pl.BlockSpec((bb, n_kv, tok, hd), lambda b: (b, 0, 0, 0))
    return pl.pallas_call(
        k_rope_kernel,
        grid=(nb // bb,),
        in_specs=[blk, tab, tab],
        out_specs=blk,
        out_shape=jax.ShapeDtypeStruct(k_proj.shape, jnp.bfloat16),
        cost_estimate=pl.CostEstimate(flops=nb * n_kv * tok * hd * 400, bytes_accessed=nb * n_kv * tok * hd * 4, transcendentals=0),
    )(k_proj, cos_tab, sin_tab)


def attn_kernel(n_ref, q_ref, k_ref, v_ref, cos_ref, sin_ref, o_ref, qa, qb, sa, sb, pa, pb, la, lb, vt, *, n_dev, q_per_kv):
    n_heads, tok, hd = q_ref.shape[1], q_ref.shape[2], q_ref.shape[3]
    n_pairs = n_heads // 2
    c = (hd ** -0.5) * LOG2E
    row_chunk = 32
    assert q_per_kv == 4

    def rope_stage(i, q_scr):
        cos_tab, sin_tab = cos_ref[0], sin_ref[0]
        for t in range(2):
            q_scr[pl.ds(t * tok, tok), :] = rope_block(q_ref[0, 2 * i + t], cos_tab, sin_tab)

    def vt_stage(i, n):
        g = (2 * i) // q_per_kv
        for j in range(n):
            vt[:, j * tok:(j + 1) * tok] = v_ref[j, 0, g].T

    def qk_stage(i, q_scr, s_scr, n):
        g = (2 * i) // q_per_kv
        s_scr[:n * tok, :] = lax.dot_general(
            k_ref[:n, 0, g].reshape(n * tok, hd), q_scr[...], (((1,), (1,)), ((), ())), preferred_element_type=jnp.float32)

    def softmax_stage(s_scr, p_scr, l_scr, n, first_masked, me):
        for t in range(2):
            cols = slice(t * tok, (t + 1) * tok)
            diff = lax.broadcasted_iota(jnp.int32, (row_chunk, tok), 0) - lax.broadcasted_iota(jnp.int32, (row_chunk, tok), 1)

            def scores(r):
                val = s_scr[r:r + row_chunk, cols]
                j = r // tok
                if j < first_masked:
                    return val
                limit = -(r % tok) if first_masked == n - 1 else me * tok - r
                return jnp.where(diff <= limit, val, -jnp.inf)

            mx = scores(0)
            for r in range(row_chunk, n * tok, row_chunk):
                mx = jnp.maximum(mx, scores(r))
            mx = jnp.max(mx, axis=0, keepdims=True)
            tot = None
            for r in range(0, n * tok, row_chunk):
                pj = jnp.exp2((scores(r) - mx) * c)
                p_scr[r:r + row_chunk, cols] = pj.astype(jnp.bfloat16)
                tot = pj if tot is None else tot + pj
            l_scr[:, cols] = jnp.broadcast_to(jnp.sum(tot, axis=0, keepdims=True), (8, tok))

    def pv_stage(i, p_scr, l_scr, n):
        acc = jnp.dot(vt[:, :n * tok], p_scr[:n * tok, :], preferred_element_type=jnp.float32)
        out = acc * (1.0 / l_scr[0:1, :])
        for t in range(2):
            o_ref[0, :, pl.ds(pl.multiple_of((2 * i + t) * hd, hd), hd)] = out[:, t * tok:(t + 1) * tok].T.astype(jnp.bfloat16)

    def run(n, lo):
        last_pair = n_pairs - 1
        rope_stage(0, qa)
        qk_stage(0, qa, sa, n)
        rope_stage(1, qb)

        def body(it, _):
            i = 2 * it
            prev = jnp.maximum(i - 1, 0)
            qk_stage(i + 1, qb, sb, n)
            rope_stage(jnp.minimum(i + 2, last_pair), qa)
            softmax_stage(sa, pa, la, n, lo - 1, me)
            pv_stage(prev, pb, lb, n)
            vt_stage(i, n)

            @pl.when(me >= 0)
            def _():
                qk_stage(jnp.minimum(i + 2, last_pair), qa, sa, n)
                rope_stage(jnp.minimum(i + 3, last_pair), qb)
                softmax_stage(sb, pb, lb, n, lo - 1, me)
                pv_stage(i, pa, la, n)

            return 0

        lax.fori_loop(0, n_pairs // 2, body, 0)
        pv_stage(last_pair, pb, lb, n)

    me = n_ref[0]
    lo = 1
    for n in VARIANTS(n_dev):
        pl.when((me + 1 >= lo) & (me < n))(functools.partial(run, n, lo))
        lo = n + 1


def attention(n_act, q, k_all, v_all, cos_tab, sin_tab):
    nb, n_heads, tok, hd = q.shape
    n_dev, _, n_kv = k_all.shape[:3]
    tab = pl.BlockSpec((1, tok, hd), lambda b, *_: (b, 0, 0))
    kv = pl.BlockSpec((n_dev, 1, n_kv, tok, hd), lambda b, *_: (0, b, 0, 0, 0))
    keys = n_dev * tok
    macs = nb * n_heads * tok * keys * hd
    return pl.pallas_call(
        functools.partial(attn_kernel, n_dev=n_dev, q_per_kv=n_heads // n_kv),
        grid_spec=pltpu.PrefetchScalarGridSpec(
            num_scalar_prefetch=1,
            grid=(nb,),
            in_specs=[pl.BlockSpec((1, n_heads, tok, hd), lambda b, *_: (b, 0, 0, 0)), kv, kv, tab, tab],
            out_specs=pl.BlockSpec((1, tok, n_heads * hd), lambda b, *_: (b, 0, 0)),
            scratch_shapes=[
                pltpu.VMEM((2 * tok, hd), jnp.bfloat16), pltpu.VMEM((2 * tok, hd), jnp.bfloat16),
                pltpu.VMEM((keys, 2 * tok), jnp.float32), pltpu.VMEM((keys, 2 * tok), jnp.float32),
                pltpu.VMEM((keys, 2 * tok), jnp.bfloat16), pltpu.VMEM((keys, 2 * tok), jnp.bfloat16),
                pltpu.VMEM((8, 2 * tok), jnp.float32), pltpu.VMEM((8, 2 * tok), jnp.float32),
                pltpu.VMEM((hd, keys), jnp.bfloat16),
            ],
        ),
        out_shape=jax.ShapeDtypeStruct((nb, tok, n_heads * hd), jnp.bfloat16),
        compiler_params=pltpu.CompilerParams(vmem_limit_bytes=60 * 1024 * 1024),
        cost_estimate=pl.CostEstimate(flops=8 * macs, bytes_accessed=2 * (2 * q.size + 2 * k_all.size), transcendentals=0),
    )(n_act, q, k_all, v_all, cos_tab, sin_tab)


def blank(shape, dtype):
    return pl.pallas_call(lambda o_ref: None, out_specs=pl.BlockSpec(memory_space=pl.ANY), out_shape=jax.ShapeDtypeStruct(shape, dtype))()


def solution(mesh):
    def per_device(hidden, positions, w_q, w_k, w_v, w_o):
        n_batch, tok = hidden.shape[0], hidden.shape[1]
        n_act = lax.axis_index('cp').astype(jnp.int32).reshape(1)
        cos_tab, sin_tab = rope_tables(positions, w_q.shape[2])
        unit = n_batch // sum(CHUNK_PARTS)
        ends = [unit * sum(CHUNK_PARTS[:i + 1]) for i in range(len(CHUNK_PARTS))]
        spans = [slice(e - unit * p, e) for e, p in zip(ends, CHUNK_PARTS)]

        def proj(x, w):
            return jnp.einsum('bsd,dhe->bshe', x, w, preferred_element_type=jnp.float32).astype(jnp.bfloat16).transpose(0, 2, 1, 3)

        k_all, v_all = [], []
        for sp in spans:
            kr = k_rope(proj(hidden[sp], w_k), cos_tab[sp], sin_tab[sp])
            k_all.append(lax.all_gather(kr, 'cp'))
            v_all.append(lax.all_gather(with_layout_constraint(proj(hidden[sp], w_v), Layout((0, 1, 2, 3))), 'cp'))
        w_o2 = w_o.reshape(-1, w_o.shape[2])
        out = blank(hidden.shape, hidden.dtype)
        for i, sp in enumerate(spans):
            q = proj(hidden[sp], w_q)
            attn = attention(n_act, q, k_all[i], v_all[i], cos_tab[sp], sin_tab[sp])
            y = jnp.einsum('bsf,fd->bsd', attn, w_o2, preferred_element_type=jnp.float32)
            y = (hidden[sp].astype(jnp.float32) + y).astype(jnp.bfloat16)
            out = lax.dynamic_update_slice(out, y, (sp.start, 0, 0))
        return out

    rep = P(None, None, None)
    return jax.shard_map(per_device, mesh=mesh, in_specs=(P('dp', 'cp', None), P('dp', 'cp'), rep, rep, rep, rep), out_specs=P('dp', 'cp', None), check_vma=False)
```
